256 devices in a mesh: seq: 16 (over z_lo, x), head: 16 (over y, z_hi, core).
Axes of the slice: x: 4, y: 4, z: 8 (z_hi: 2, z_lo: 4; z = z_hi * 4 + z_lo), core: 2. Of those that a mesh axis runs over, the one named last changes fastest.
Arguments:
- video_q: bfloat16 [8192, 4096], P(('seq', 'head')), may hold values from -200 to 200
- video_k: bfloat16 [8192, 4096], P(('seq', 'head')), may hold values from -6 to 6
- video_v: bfloat16 [8192, 4096], P(('seq', 'head')), may hold values from -6 to 6
- text_k: bfloat16 [512, 4096], P(None, 'head'), may hold values from -6 to 6
- text_v: bfloat16 [512, 4096], P(None, 'head'), may hold values from -6 to 6
- out_weight: bfloat16 [4096, 5120], P('head'), may hold values from -0.09375 to 0.09375
Outputs:
- video_out: bfloat16 [8192, 5120], P(('seq', 'head'))
The draws below stay inside these ranges and needn't reach their ends.
All inputs are finite; a program needn't handle non-finite values.
Results may differ from the reference program's by a relative error of at most 0.018.
Values may be sent and summed in bfloat16 or wider, within the bound.
A program may use at most 128 MiB of HBM per device.

```python
import jax
import jax.numpy as jnp
from jax import lax

D = 5120
HEADS = 32
HD = 128
TEXT = 512
TOKENS = 8192
N_HEAD = 16


def paired_draw(key):
    shape = (TOKENS, HEADS * HD)
    key_rows = jnp.clip(jax.random.normal(jax.random.fold_in(key, 11), shape, jnp.float32), -6.0, 6.0)
    queries = jnp.clip(jax.random.normal(jax.random.fold_in(key, 12), shape, jnp.float32), -6.0, 6.0)
    return (queries, key_rows)


def draw_video_q(key, part):
    queries, key_rows = paired_draw(key)
    return queries.astype(jnp.bfloat16)


def draw_video_k(key, part):
    queries, key_rows = paired_draw(key)
    return key_rows.astype(jnp.bfloat16)


def block_levels(rng, extent, pieces, low, largest):
    def one(position, blocks):
        draws = jax.random.uniform(jax.random.fold_in(jax.random.fold_in(rng, 6), position), (blocks,), jnp.float32, low / len(pieces), largest / len(pieces))
        return jnp.repeat(jnp.exp(draws), extent[position] // blocks).reshape((-1,) + (1,) * (len(extent) - position - 1))

    loudness = one(*pieces[0])
    for cut in pieces[1:]:
        loudness = loudness * one(*cut)
    return loudness


def normal_values(own_key, shape, scale, most, split=(), dtype=jnp.bfloat16):
    values = jax.random.normal(own_key, shape, jnp.float32) * scale
    if len(split) > 0:
        values = block_levels(own_key, shape, split, -0.22, 0.18) * values
    return jnp.clip(values, min=-most, max=most).astype(dtype)


def setup_inputs(seed: int = 0) -> dict:
    arg_keys = jax.random.split(jax.random.key(seed), 7)
    video_q = draw_video_q(jax.random.fold_in(arg_keys[6], 71), 0)
    video_k = draw_video_k(jax.random.fold_in(arg_keys[6], 71), 0)
    video_v = normal_values(arg_keys[2], (TOKENS, HEADS * HD), 1.0, 6.0, ((0, 256),))
    text_k = normal_values(arg_keys[3], (TEXT, HEADS * HD), 1.0, 6.0, ((1, 16),))
    text_v = normal_values(arg_keys[4], (TEXT, HEADS * HD), 1.0, 6.0, ((1, 16),))
    out_weight = normal_values(arg_keys[5], (HEADS * HD, D), (HEADS * HD) ** -0.5, 0.09375, ((0, 16),))
    return {"video_q": video_q, "video_k": video_k, "video_v": video_v, "text_k": text_k, "text_v": text_v, "out_weight": out_weight}


def head_output(operands):
    queries, key_rows, value_rows = operands
    scores = jnp.dot(queries, key_rows.T, preferred_element_type=jnp.float32) * (HD ** -0.5)
    row_max = jnp.max(scores, axis=1, keepdims=True)
    weights = jnp.exp(scores - row_max).astype(jnp.bfloat16)
    totals = jnp.sum(weights.astype(jnp.float32), axis=1, keepdims=True)
    summed = jnp.dot(weights, value_rows, preferred_element_type=jnp.float32)
    return (summed / totals).astype(jnp.bfloat16)


def split_heads(array):
    return array.reshape(array.shape[0], HEADS, HD).transpose(1, 0, 2)


def reference(video_q, video_k, video_v, text_k, text_v, out_weight):
    tokens = video_q.shape[0]
    all_keys = jnp.concatenate([split_heads(video_k), split_heads(text_k)], axis=1)
    all_values = jnp.concatenate([split_heads(video_v), split_heads(text_v)], axis=1)
    attended = lax.map(head_output, (split_heads(video_q), all_keys, all_values))
    attended = attended.transpose(1, 0, 2).reshape(tokens, HEADS * HD)
    group_width = HEADS * HD // N_HEAD
    group_inputs = attended.reshape(tokens, N_HEAD, group_width).transpose(1, 0, 2)
    weight_groups = out_weight.reshape(N_HEAD, group_width, D)

    def add_group(summed_out, operands):
        part_in, part_weight = operands
        partial_out = jnp.dot(part_in, part_weight, preferred_element_type=jnp.float32).astype(jnp.bfloat16)
        partial_out = lax.optimization_barrier(partial_out)
        return summed_out + partial_out.astype(jnp.float32), None

    summed_out, unused = lax.scan(add_group, jnp.zeros((tokens, D), jnp.float32), (group_inputs, weight_groups))
    return summed_out.astype(jnp.bfloat16)
```

```python
import functools
import math

import jax
import jax.numpy as jnp
from jax import lax
from jax.experimental import pallas as pl
from jax.experimental.pallas import tpu as pltpu
from jax.sharding import PartitionSpec as P

HD = 128
C2 = HD ** (-0.5) * math.log2(math.e)
BF = jnp.bfloat16
F32 = jnp.float32
MESH = pl.DeviceIdType.MESH
COLS = 1280
CW = 256
NCH = COLS // CW


def kernel(
    q_hbm, k_hbm, v_hbm, tk_hbm, tv_hbm, w_hbm, out_ref,
    qs, ks, vs, qbuf, kbuf, vbuf, tbuf, wbuf, abuf, att, acc, m_ref, l_ref,
    psend, pown, zbuf, osend,
    s_loc, p1_send, p1_recv, x_send, x_recv, d_send, d_recv, t_send, t_recv,
    w_send, w_recv, wd_send, wd_recv, a_send, a_recv, b_send, b_recv,
    z_send, z_recv, o_send, o_recv,
):
    s, h = lax.axis_index("seq"), lax.axis_index("head")
    x, zl = s % 4, s // 4
    y, zh, c = h // 4, (h // 2) % 2, h % 2
    z = zh * 4 + zl
    p = y * 8 + z

    def dev(x1, y1, zh1, zl1, c1):
        return (zl1 * 4 + x1, y1 * 4 + zh1 * 2 + c1)

    left, right = (x + 3) % 4, (x + 1) % 4

    stage = []
    for i, (src, dst) in enumerate(((k_hbm, ks), (v_hbm, vs), (q_hbm, qs))):
        cp = pltpu.make_async_copy(src, dst, s_loc.at[i])
        cp.start()
        stage.append(cp)

    barrier = pltpu.get_barrier_semaphore()

    def greet(i, carry):
        pp = (p + i) % 32
        pl.semaphore_signal(
            barrier, inc=1, device_id=dev(x, pp // 8, (pp // 4) % 2, pp % 4, c), device_id_type=MESH
        )
        return carry

    lax.fori_loop(1, 32, greet, 0)
    for d in (dev(left, y, zh, zl, c), dev(right, y, zh, zl, c), dev(x, y, zh, zl, 1 - c)):
        pl.semaphore_signal(barrier, inc=1, device_id=d, device_id_type=MESH)
    pl.semaphore_wait(barrier, 34)

    def remote(src, dst, ss, rs, device):
        return pltpu.make_async_remote_copy(
            src_ref=src, dst_ref=dst, send_sem=ss, recv_sem=rs, device_id=device, device_id_type=MESH
        )

    partner = dev(x, y, zh, zl, 1 - c)
    krow = pl.multiple_of(p * 32, 32)
    qrow = pl.multiple_of(zl * 256 + (zh * 4 + y) * 32, 32)
    dests = (
        kbuf.at[0, c, pl.ds(krow, 32)],
        vbuf.at[0, c, pl.ds(krow, 32)],
        qbuf.at[pl.ds(qrow, 32)],
    )
    own = []
    for i, src in enumerate((ks, vs, qs)):
        stage[i].wait()

        def send(j, carry, i=i, src=src):
            pp = (p + j) % 32
            col = pl.multiple_of(pp * 128, 128)
            remote(
                src.at[:, pl.ds(col, 128)], dests[i], p1_send.at[i], p1_recv.at[i],
                dev(x, pp // 8, (pp // 4) % 2, pp % 4, c),
            ).start()
            return carry

        lax.fori_loop(1, 32, send, 0)
        cp = pltpu.make_async_copy(
            src.at[:, pl.ds(pl.multiple_of(p * 128, 128), 128)], dests[i], s_loc.at[3 + i]
        )
        cp.start()
        own.append(cp)

    tcol = pl.multiple_of((zl % 2) * 128, 128)
    texts = []
    for i, src in enumerate((tk_hbm, tv_hbm)):
        piece = src.at[:, pl.ds(tcol, 128)]
        cp = remote(piece, tbuf.at[i, c], t_send.at[i], t_recv.at[i], partner)
        cp.start()
        mine = pltpu.make_async_copy(piece, tbuf.at[i, c], s_loc.at[6 + i])
        mine.start()
        texts.append((cp, mine))

    wrow = pl.ds(pl.multiple_of(c * 256, 256), 256)

    def wcols(y1):
        return w_hbm.at[:, pl.ds(pl.multiple_of(y1 * COLS, 128), COLS)]

    wown = pltpu.make_async_copy(wcols(y), wbuf.at[y, wrow], s_loc.at[8])
    wown.start()
    wd = [remote(wcols(y), wbuf.at[y, wrow], wd_send.at[0], wd_recv.at[0], partner)]
    wd[0].start()

    def share(buf, slot):
        return buf.at[slot, c]

    def total_wait(buf, sem):
        pltpu.make_async_copy(buf, buf, sem).wait()

    bufs = (kbuf, vbuf)
    xs = {}
    ds = {}

    def send_x(i, src_slot, dst_slot, to):
        cp = remote(
            share(bufs[i], src_slot), share(bufs[i], dst_slot),
            x_send.at[i, dst_slot], x_recv.at[i, dst_slot], dev(to, y, zh, zl, c),
        )
        cp.start()
        xs[(i, dst_slot)] = cp

    def send_d(i, slot):
        cp = remote(
            share(bufs[i], slot), share(bufs[i], slot), d_send.at[i, slot], d_recv.at[i, slot], partner
        )
        cp.start()
        ds[(i, slot)] = cp

    for i in (0, 1):
        own[i].wait()
        total_wait(bufs[i].at[0, c, pl.ds(0, 31 * 32)], p1_recv.at[i])
        send_x(i, 0, 3, right)
        send_x(i, 0, 1, left)
        send_d(i, 0)

    ws = []
    for dy in range(1, 4):
        y1 = (y + dy) % 4
        cp = remote(wcols(y1), wbuf.at[y, wrow], w_send.at[dy], w_recv.at[dy], dev(x, y1, zh, zl, c))
        cp.start()
        ws.append(cp)

    own[2].wait()
    total_wait(qbuf.at[pl.ds(0, 31 * 32)], p1_recv.at[2])
    for cp, mine in texts:
        mine.wait()
        cp.wait_recv()

    def step(row, keys, values, first):
        rows = pl.ds(row, 256)
        sc = lax.dot_general(
            qbuf[rows, :], keys, (((1,), (1,)), ((), ())), preferred_element_type=F32
        )
        m_cur = jnp.max(sc, axis=1, keepdims=True)
        if first:
            m_new = m_cur
        else:
            m_old = m_ref[rows, :1]
            m_new = jnp.maximum(m_old, m_cur)
        w = jnp.exp2((sc - m_new) * C2)
        tot = jnp.sum(w, axis=1, keepdims=True)
        o = jnp.dot(w.astype(BF), values, preferred_element_type=F32)
        if first:
            acc[rows, :] = o
            l_ref[rows, :] = jnp.broadcast_to(tot, (256, 128))
        else:
            al = jnp.exp2((m_old - m_new) * C2)
            acc[rows, :] = acc[rows, :] * al + o
            l_ref[rows, :] = l_ref[rows, :] * al + tot
        m_ref[rows, :] = jnp.broadcast_to(m_new, (256, 128))

    src_core = zl // 2

    def text_block(qi, carry):
        step(pl.multiple_of(qi * 256, 256), tbuf[0, src_core], tbuf[1, src_core], True)
        return carry

    lax.fori_loop(0, 4, text_block, 0)

    def video_block(row, slot):
        for core in range(2):
            step(row, kbuf[slot, core], vbuf[slot, core], False)

    def all_rows(slot):
        def one(qi, carry):
            video_block(pl.multiple_of(qi * 256, 256), slot)
            return carry

        lax.fori_loop(0, 4, one, 0)

    for i in (0, 1):
        ds[(i, 0)].wait_recv()
    all_rows(0)

    xs[(0, 3)].wait_recv()
    send_x(0, 3, 2, right)
    send_d(0, 3)
    xs[(0, 1)].wait_recv()
    send_d(0, 1)
    xs[(1, 1)].wait_recv()
    send_x(1, 1, 2, left)
    send_d(1, 1)
    xs[(1, 3)].wait_recv()
    send_d(1, 3)
    for i in (0, 1):
        ds[(i, 1)].wait_recv()
    all_rows(1)
    for i in (0, 1):
        ds[(i, 3)].wait_recv()
    all_rows(3)

    wown.wait()
    for dy in range(1, 4):
        ws[dy - 1].wait_recv()
        piece = wbuf.at[(y + 4 - dy) % 4, wrow]
        cp = remote(piece, piece, wd_send.at[dy], wd_recv.at[dy], partner)
        cp.start()
        wd.append(cp)

    for i in (0, 1):
        xs[(i, 2)].wait_recv()
        send_d(i, 2)
    for i in (0, 1):
        ds[(i, 2)].wait_recv()

    bs = []
    asend = []

    def forward(d):
        cols = pl.ds(pl.multiple_of(((zl + 4 - d) % 4) * 128, 128), 128)
        piece = abuf.at[y, :, cols]
        for dy in range(1, 4):
            cp = remote(
                piece, piece, b_send.at[d, dy], b_recv.at[d, dy], dev(x, (y + dy) % 4, zh, zl, c)
            )
            cp.start()
            bs.append(cp)

    mycols = pl.ds(pl.multiple_of(zl * 128, 128), 128)
    for n, d in enumerate((1, 2, 3, 0)):
        zl1 = (zl + d) % 4
        row = pl.multiple_of(zl1 * 256, 256)
        rows = pl.ds(row, 256)
        video_block(row, 2)
        res = (acc[rows, :] / l_ref[rows, :]).astype(BF)
        if d:
            att[rows, :] = res
            cp = remote(
                att.at[rows], abuf.at[y, :, mycols], a_send.at[d], a_recv.at[d], dev(x, y, zh, zl1, c)
            )
            cp.start()
            asend.append(cp)
            if n:
                asend[n - 1].wait_recv()
                forward(n)
        else:
            abuf[y, :, mycols] = res
            asend[2].wait_recv()
            forward(3)
            forward(0)

    for cp in wd:
        cp.wait_recv()
    for cp in bs:
        cp.wait_recv()

    def part(row, n):
        tot = None
        for yy in range(4):
            t = jnp.dot(
                abuf[yy, pl.ds(row, 128), :], wbuf[yy, :, n * CW : (n + 1) * CW],
                preferred_element_type=F32,
            )
            tot = t if tot is None else tot + t
        return tot

    away = pl.multiple_of((1 - zh) * 128, 128)
    home = pl.multiple_of(zh * 128, 128)
    zs = []
    for n in range(NCH):
        psend[n] = part(away, n).astype(BF)
        cp = remote(psend.at[n], zbuf.at[n], z_send.at[n], z_recv.at[n], dev(x, y, 1 - zh, zl, c))
        cp.start()
        zs.append(cp)
    for n in range(NCH):
        pown[n] = part(home, n)
    os = []
    for n in range(NCH):
        zs[n].wait_recv()
        osend[n] = (pown[n] + zbuf[n].astype(F32)).astype(BF)
        for dy in range(1, 4):
            y1 = (y + dy) % 4
            cp = remote(
                osend.at[n, pl.ds(pl.multiple_of(y1 * 32, 32), 32)],
                out_ref.at[:, pl.ds(pl.multiple_of(y * COLS + n * CW, 128), CW)],
                o_send.at[n, dy], o_recv.at[n, dy], dev(x, y1, zh, zl, c),
            )
            cp.start()
            os.append(cp)
        out_ref[:, pl.ds(pl.multiple_of(y * COLS + n * CW, 128), CW)] = osend[
            n, pl.ds(pl.multiple_of(y * 32, 32), 32), :
        ]

    for cp in os:
        cp.wait_recv()
    for i, src in enumerate((kbuf.at[0, c], vbuf.at[0, c], qbuf)):
        total_wait(src.at[pl.ds(0, 31 * 32)], p1_send.at[i])
    for cp in (
        [t[0] for t in texts] + ws + wd + list(xs.values()) + list(ds.values()) + asend + bs + zs + os
    ):
        cp.wait_send()


def body(*args):
    dma = pltpu.SemaphoreType.DMA
    vm = pltpu.VMEM
    return pl.pallas_call(
        kernel,
        out_shape=jax.ShapeDtypeStruct((32, 5120), BF),
        in_specs=[pl.BlockSpec(memory_space=pl.ANY)] * 6,
        out_specs=pl.BlockSpec(memory_space=pltpu.VMEM),
        scratch_shapes=[
            vm((32, 4096), BF), vm((32, 4096), BF), vm((32, 4096), BF),
            vm((1024, 128), BF), vm((4, 2, 1024, 128), BF), vm((4, 2, 1024, 128), BF),
            vm((2, 2, 512, 128), BF), vm((4, 512, COLS), BF), vm((4, 256, 512), BF),
            vm((1024, 128), BF), vm((1024, 128), F32), vm((1024, 128), F32), vm((1024, 128), F32),
            vm((NCH, 128, CW), BF), vm((NCH, 128, CW), F32), vm((NCH, 128, CW), BF), vm((NCH, 128, CW), BF),
            dma((9,)), dma((3,)), dma((3,)), dma((2, 4)), dma((2, 4)), dma((2, 4)), dma((2, 4)),
            dma((2,)), dma((2,)), dma((4,)), dma((4,)), dma((4,)), dma((4,)),
            dma((4,)), dma((4,)), dma((4, 4)), dma((4, 4)),
            dma((NCH,)), dma((NCH,)), dma((NCH, 4)), dma((NCH, 4)),
        ],
        compiler_params=pltpu.CompilerParams(
            collective_id=0, has_side_effects=True, vmem_limit_bytes=60 * 1024 * 1024
        ),
    )(*args)


def solution(mesh):
    rows = P(("seq", "head"), None)
    in_specs = (rows, rows, rows, P(None, "head"), P(None, "head"), P("head", None))
    return jax.shard_map(body, mesh=mesh, in_specs=in_specs, out_specs=rows, check_vma=False)
```

```python
import functools
import math

import jax
import jax.numpy as jnp
from jax import lax
from jax.experimental import pallas as pl
from jax.experimental.pallas import tpu as pltpu
from jax.sharding import PartitionSpec as P

HD = 128
C2 = HD ** (-0.5) * math.log2(math.e)
BF = jnp.bfloat16
F32 = jnp.float32
MESH = pl.DeviceIdType.MESH
COLS = 1280
CW = 256
NCH = COLS // CW


def kernel(
    q_hbm, k_hbm, v_hbm, tk_hbm, tv_hbm, w_hbm, out_ref,
    qs, ks, vs, qbuf, kbuf, vbuf, tbuf, wbuf, abuf, att, acc, m_ref, l_ref,
    psend, pown, zbuf, osend,
    s_loc, p1_send, p1_recv, x_send, x_recv, d_send, d_recv, t_send, t_recv,
    w_send, w_recv, wd_send, wd_recv, a_send, a_recv, b_send, b_recv,
    z_send, z_recv, o_send, o_recv,
):
    s, h = lax.axis_index("seq"), lax.axis_index("head")
    x, zl = s % 4, s // 4
    y, zh, c = h // 4, (h // 2) % 2, h % 2
    z = zh * 4 + zl
    p = y * 8 + z

    def dev(x1, y1, zh1, zl1, c1):
        return (zl1 * 4 + x1, y1 * 4 + zh1 * 2 + c1)

    left, right = (x + 3) % 4, (x + 1) % 4

    stage = []
    for i, (src, dst) in enumerate(((k_hbm, ks), (v_hbm, vs), (q_hbm, qs))):
        cp = pltpu.make_async_copy(src, dst, s_loc.at[i])
        cp.start()
        stage.append(cp)

    barrier = pltpu.get_barrier_semaphore()

    def greet(i, carry):
        pp = (p + i) % 32
        pl.semaphore_signal(
            barrier, inc=1, device_id=dev(x, pp // 8, (pp // 4) % 2, pp % 4, c), device_id_type=MESH
        )
        return carry

    lax.fori_loop(1, 32, greet, 0)
    for d in (dev(left, y, zh, zl, c), dev(right, y, zh, zl, c), dev(x, y, zh, zl, 1 - c)):
        pl.semaphore_signal(barrier, inc=1, device_id=d, device_id_type=MESH)
    pl.semaphore_wait(barrier, 34)

    def remote(src, dst, ss, rs, device):
        return pltpu.make_async_remote_copy(
            src_ref=src, dst_ref=dst, send_sem=ss, recv_sem=rs, device_id=device, device_id_type=MESH
        )

    partner = dev(x, y, zh, zl, 1 - c)
    qrow = pl.multiple_of(zh * 512 + zl * 128 + y * 32, 32)
    stages = {0: ks, 1: vs, 2: qs}
    bufs = (kbuf, vbuf)

    def send_half(i, half):
        def send(j, carry):
            dz, dy = (j // 4) * 2 + half, j % 4
            y1, z1 = (y + dy) % 4, (z + dz) % 8
            col = pl.multiple_of((y1 * 8 + z1) * 128, 128)
            row = pl.multiple_of(half * 512 + j * 32, 32)
            dst = qbuf.at[pl.ds(qrow, 32)] if i == 2 else bufs[i].at[0, c, pl.ds(row, 32)]
            remote(
                stages[i].at[:, pl.ds(col, 128)], dst, p1_send.at[i, half], p1_recv.at[i, half],
                dev(x, y1, z1 // 4, z1 % 4, c),
            ).start()
            return carry

        lax.fori_loop(1 - half, 16, send, 0)

    mycol = pl.ds(pl.multiple_of(p * 128, 128), 128)
    own = {}
    for i, half in ((0, 0), (1, 0), (2, 0), (2, 1), (0, 1), (1, 1)):
        if half == 0:
            stage[i].wait()
        send_half(i, half)
        if half == 0:
            dst = qbuf.at[pl.ds(qrow, 32)] if i == 2 else bufs[i].at[0, c, pl.ds(0, 32)]
            cp = pltpu.make_async_copy(stages[i].at[:, mycol], dst, s_loc.at[3 + i])
            cp.start()
            own[i] = cp

    tcol = pl.multiple_of((zl % 2) * 128, 128)
    texts = []
    for i, src in enumerate((tk_hbm, tv_hbm)):
        piece = src.at[:, pl.ds(tcol, 128)]
        cp = remote(piece, tbuf.at[i, c], t_send.at[i], t_recv.at[i], partner)
        cp.start()
        mine = pltpu.make_async_copy(piece, tbuf.at[i, c], s_loc.at[6 + i])
        mine.start()
        texts.append((cp, mine))

    wrow = pl.ds(pl.multiple_of(c * 256, 256), 256)

    def wcols(y1):
        return w_hbm.at[:, pl.ds(pl.multiple_of(y1 * COLS, 128), COLS)]

    wown = pltpu.make_async_copy(wcols(y), wbuf.at[y, wrow], s_loc.at[8])
    wown.start()
    wd = [remote(wcols(y), wbuf.at[y, wrow], wd_send.at[0], wd_recv.at[0], partner)]
    wd[0].start()
    ws = {}
    for dy in (2, 1, 3):
        y1 = (y + dy) % 4
        ws[dy] = remote(wcols(y1), wbuf.at[y, wrow], w_send.at[dy], w_recv.at[dy], dev(x, y1, zh, zl, c))
        ws[dy].start()

    def total_wait(buf, sem):
        pltpu.make_async_copy(buf, buf, sem).wait()

    xs, ds = {}, {}

    def share(i, half, slot):
        return bufs[i].at[slot, c, pl.ds(half * 512, 512)]

    def send_x(i, half, src_slot, dst_slot, to):
        cp = remote(
            share(i, half, src_slot), share(i, half, dst_slot),
            x_send.at[i, half, dst_slot], x_recv.at[i, half, dst_slot], dev(to, y, zh, zl, c),
        )
        cp.start()
        xs[(i, half, dst_slot)] = cp

    def send_d(i, half, slot):
        cp = remote(
            share(i, half, slot), share(i, half, slot),
            d_send.at[i, half, slot], d_recv.at[i, half, slot], partner,
        )
        cp.start()
        ds[(i, half, slot)] = cp

    def arrive_own(i, half):
        if half == 0:
            own[i].wait()
        n = 480 if half == 0 else 512
        total_wait(bufs[i].at[0, c, pl.ds(0, n)], p1_recv.at[i, half])
        send_x(i, half, 0, 3, right)
        send_x(i, half, 0, 1, left)
        send_d(i, half, 0)

    def arrive_near(i, half):
        first, second = (3, 1) if i == 0 else (1, 3)
        xs[(i, half, first)].wait_recv()
        send_x(i, half, first, 2, right if i == 0 else left)
        send_d(i, half, first)
        xs[(i, half, second)].wait_recv()
        send_d(i, half, second)

    def arrive_far(half):
        for i in (0, 1):
            xs[(i, half, 2)].wait_recv()
            send_d(i, half, 2)

    def arrive_core(half, slot):
        for i in (0, 1):
            ds[(i, half, slot)].wait_recv()

    def step(row, pieces, first):
        rows = pl.ds(row, 256)
        q = qbuf[rows, :]
        scs = [
            lax.dot_general(q, kk(), (((1,), (1,)), ((), ())), preferred_element_type=F32)
            for kk, vv in pieces
        ]
        m_new = functools.reduce(jnp.maximum, [jnp.max(sc, axis=1, keepdims=True) for sc in scs])
        if not first:
            m_old = m_ref[rows, :1]
            m_new = jnp.maximum(m_old, m_new)
        tot, o = 0.0, 0.0
        for sc, (kk, vv) in zip(scs, pieces):
            w = jnp.exp2((sc - m_new) * C2)
            tot = tot + jnp.sum(w, axis=1, keepdims=True)
            o = o + jnp.dot(w.astype(BF), vv(), preferred_element_type=F32)
        if first:
            acc[rows, :] = o
            l_ref[rows, :] = jnp.broadcast_to(tot, (256, 128))
        else:
            al = jnp.exp2((m_old - m_new) * C2)
            acc[rows, :] = acc[rows, :] * al + o
            l_ref[rows, :] = l_ref[rows, :] * al + tot
        m_ref[rows, :] = jnp.broadcast_to(m_new, (256, 128))

    src_core = zl // 2
    text_piece = (lambda: tbuf[0, src_core], lambda: tbuf[1, src_core])

    def video_pieces(half, slot):
        hr = pl.ds(half * 512, 512)
        return [
            (lambda core=core: kbuf[slot, core, hr], lambda core=core: vbuf[slot, core, hr])
            for core in range(2)
        ]

    def all_rows(pieces, first=False):
        def one(qi, carry):
            step(pl.multiple_of(qi * 256, 256), pieces, first)
            return carry

        lax.fori_loop(0, 4, one, 0)

    arrive_own(0, 0)
    arrive_own(1, 0)
    arrive_near(0, 0)
    arrive_near(1, 0)
    own[2].wait()
    total_wait(qbuf.at[pl.ds(0, 480)], p1_recv.at[2, 0])
    total_wait(qbuf.at[pl.ds(0, 512)], p1_recv.at[2, 1])
    for cp, mine in texts:
        mine.wait()
        cp.wait_recv()
    all_rows([text_piece], True)
    arrive_core(0, 0)
    all_rows(video_pieces(0, 0))
    arrive_own(0, 1)
    arrive_far(0)
    arrive_core(0, 1)
    all_rows(video_pieces(0, 1))
    arrive_own(1, 1)
    arrive_core(0, 3)
    all_rows(video_pieces(0, 3))
    arrive_near(0, 1)
    arrive_core(0, 2)
    all_rows(video_pieces(0, 2))
    arrive_near(1, 1)
    arrive_core(1, 0)
    all_rows(video_pieces(1, 0))
    arrive_core(1, 1)
    all_rows(video_pieces(1, 1))
    arrive_far(1)
    arrive_core(1, 3)
    all_rows(video_pieces(1, 3))

    wown.wait()
    for dy in (2, 1, 3):
        ws[dy].wait_recv()
        piece = wbuf.at[(y + 4 - dy) % 4, wrow]
        cp = remote(piece, piece, wd_send.at[dy], wd_recv.at[dy], partner)
        cp.start()
        wd.append(cp)
    arrive_core(1, 2)

    aas, bs = {}, {}
    mycols = pl.ds(pl.multiple_of(zl * 128, 128), 128)

    def last_rows(zhalf, k):
        row = pl.multiple_of(zhalf * 512 + k * 256, 256)
        step(row, video_pieces(1, 2), False)
        rows = pl.ds(row, 256)
        att[rows, :] = (acc[rows, :] / l_ref[rows, :]).astype(BF)

    def send_att(zhalf, k):
        for d in range(1, 4):
            zl1 = (zl + d) % 4
            rows = pl.ds(pl.multiple_of(zhalf * 512 + zl1 * 128, 128), 128)
            cp = remote(
                att.at[rows], abuf.at[zhalf, y, :, mycols], a_send.at[k, d], a_recv.at[k, d],
                dev(x, y, zh, zl1, c),
            )
            cp.start()
            aas[(k, d)] = cp
        rows = pl.ds(pl.multiple_of(zhalf * 512 + zl * 128, 128), 128)
        abuf[zhalf, y, :, mycols] = att[rows, :]

    def send_b(zhalf, k):
        for d in range(1, 4):
            aas[(k, d)].wait_recv()
        piece = abuf.at[zhalf, y]
        for dy in (2, 1, 3):
            cp = remote(
                piece, piece, b_send.at[k, dy], b_recv.at[k, dy], dev(x, (y + dy) % 4, zh, zl, c)
            )
            cp.start()
            bs[(k, dy)] = cp

    away, home = 1 - zh, zh
    last_rows(away, 0)
    last_rows(away, 1)
    send_att(away, 0)
    last_rows(home, 0)
    last_rows(home, 1)
    send_att(home, 1)
    send_b(away, 0)
    send_b(home, 1)

    for cp in wd:
        cp.wait_recv()

    def part(zhalf, n):
        tot = None
        for yy in range(4):
            t = jnp.dot(
                abuf[zhalf, yy], wbuf[yy, :, n * CW : (n + 1) * CW], preferred_element_type=F32
            )
            tot = t if tot is None else tot + t
        return tot

    for dy in range(1, 4):
        bs[(0, dy)].wait_recv()
    zs = []
    for n in range(NCH):
        psend[n] = part(away, n).astype(BF)
        cp = remote(psend.at[n], zbuf.at[n], z_send.at[n], z_recv.at[n], dev(x, y, 1 - zh, zl, c))
        cp.start()
        zs.append(cp)
    for dy in range(1, 4):
        bs[(1, dy)].wait_recv()
    for n in range(NCH):
        pown[n] = part(home, n)
    os = []
    for n in range(NCH):
        zs[n].wait_recv()
        osend[n] = (pown[n] + zbuf[n].astype(F32)).astype(BF)
        for dy in (2, 1, 3):
            y1 = (y + dy) % 4
            cp = remote(
                osend.at[n, pl.ds(pl.multiple_of(y1 * 32, 32), 32)],
                out_ref.at[:, pl.ds(pl.multiple_of(y * COLS + n * CW, 128), CW)],
                o_send.at[n, dy], o_recv.at[n, dy], dev(x, y1, zh, zl, c),
            )
            cp.start()
            os.append(cp)
        out_ref[:, pl.ds(pl.multiple_of(y * COLS + n * CW, 128), CW)] = osend[
            n, pl.ds(pl.multiple_of(y * 32, 32), 32), :
        ]

    for cp in os:
        cp.wait_recv()
    for i in range(3):
        for half in range(2):
            n = 480 if half == 0 else 512
            total_wait(qbuf.at[pl.ds(0, n)], p1_send.at[i, half])
    for cp in (
        [t[0] for t in texts] + list(ws.values()) + wd + list(xs.values()) + list(ds.values())
        + list(aas.values()) + list(bs.values()) + zs + os
    ):
        cp.wait_send()


def body(*args):
    dma = pltpu.SemaphoreType.DMA
    vm = pltpu.VMEM
    return pl.pallas_call(
        kernel,
        out_shape=jax.ShapeDtypeStruct((32, 5120), BF),
        in_specs=[pl.BlockSpec(memory_space=pl.ANY)] * 6,
        out_specs=pl.BlockSpec(memory_space=pltpu.VMEM),
        scratch_shapes=[
            vm((32, 4096), BF), vm((32, 4096), BF), vm((32, 4096), BF),
            vm((1024, 128), BF), vm((4, 2, 1024, 128), BF), vm((4, 2, 1024, 128), BF),
            vm((2, 2, 512, 128), BF), vm((4, 512, COLS), BF), vm((2, 4, 128, 512), BF),
            vm((1024, 128), BF), vm((1024, 128), F32), vm((1024, 128), F32), vm((1024, 128), F32),
            vm((NCH, 128, CW), BF), vm((NCH, 128, CW), F32), vm((NCH, 128, CW), BF), vm((NCH, 128, CW), BF),
            dma((9,)), dma((3, 2)), dma((3, 2)), dma((2, 2, 4)), dma((2, 2, 4)), dma((2, 2, 4)), dma((2, 2, 4)),
            dma((2,)), dma((2,)), dma((4,)), dma((4,)), dma((4,)), dma((4,)),
            dma((2, 4)), dma((2, 4)), dma((2, 4)), dma((2, 4)),
            dma((NCH,)), dma((NCH,)), dma((NCH, 4)), dma((NCH, 4)),
        ],
        compiler_params=pltpu.CompilerParams(
            collective_id=0, has_side_effects=True, vmem_limit_bytes=60 * 1024 * 1024
        ),
    )(*args)


def solution(mesh):
    rows = P(("seq", "head"), None)
    in_specs = (rows, rows, rows, P(None, "head"), P(None, "head"), P("head", None))
    return jax.shard_map(body, mesh=mesh, in_specs=in_specs, out_specs=rows, check_vma=False)
```

```python
import functools
import math

import jax
import jax.numpy as jnp
from jax import lax
from jax.experimental import pallas as pl
from jax.experimental.pallas import tpu as pltpu
from jax.sharding import PartitionSpec as P

HD = 128
C2 = HD ** (-0.5) * math.log2(math.e)
BF = jnp.bfloat16
F32 = jnp.float32
MESH = pl.DeviceIdType.MESH
COLS = 1280
QB = 512
CW = 256
NCH = COLS // CW


def kernel(
    q_hbm, k_hbm, v_hbm, tk_hbm, tv_hbm, w_hbm, out_ref,
    qs, ks, vs, qbuf, kbuf, vbuf, tbuf, wbuf, abuf, att, acc, m_ref, l_ref,
    psend, pown, zbuf, osend,
    s_loc, p1_send, p1_recv, x_send, x_recv, d_send, d_recv, t_send, t_recv,
    w_send, w_recv, wd_send, wd_recv, a_send, a_recv, b_send, b_recv,
    z_send, z_recv, o_send, o_recv,
):
    s, h = lax.axis_index("seq"), lax.axis_index("head")
    x, zl = s % 4, s // 4
    y, zh, c = h // 4, (h // 2) % 2, h % 2
    z = zh * 4 + zl
    p = y * 8 + z

    def dev(x1, y1, zh1, zl1, c1):
        return (zl1 * 4 + x1, y1 * 4 + zh1 * 2 + c1)

    left, right = (x + 3) % 4, (x + 1) % 4

    stage = []
    for i, (src, dst) in enumerate(((k_hbm, ks), (v_hbm, vs), (q_hbm, qs))):
        cp = pltpu.make_async_copy(src, dst, s_loc.at[i])
        cp.start()
        stage.append(cp)

    barrier = pltpu.get_barrier_semaphore()

    def greet(i, carry):
        pp = (p + i) % 32
        pl.semaphore_signal(
            barrier, inc=1, device_id=dev(x, pp // 8, (pp // 4) % 2, pp % 4, c), device_id_type=MESH
        )
        return carry

    lax.fori_loop(1, 32, greet, 0)
    for d in (dev(left, y, zh, zl, c), dev(right, y, zh, zl, c), dev(x, y, zh, zl, 1 - c)):
        pl.semaphore_signal(barrier, inc=1, device_id=d, device_id_type=MESH)
    pl.semaphore_wait(barrier, 34)

    def remote(src, dst, ss, rs, device):
        return pltpu.make_async_remote_copy(
            src_ref=src, dst_ref=dst, send_sem=ss, recv_sem=rs, device_id=device, device_id_type=MESH
        )

    partner = dev(x, y, zh, zl, 1 - c)
    qrow = pl.multiple_of(zh * 512 + zl * 128 + y * 32, 32)
    stages = {0: ks, 1: vs, 2: qs}
    bufs = (kbuf, vbuf)

    def send_half(i, half):
        def send(j, carry):
            dz, dy = (j // 4) * 2 + half, j % 4
            y1, z1 = (y + dy) % 4, (z + dz) % 8
            col = pl.multiple_of((y1 * 8 + z1) * 128, 128)
            row = pl.multiple_of(half * 512 + j * 32, 32)
            dst = qbuf.at[pl.ds(qrow, 32)] if i == 2 else bufs[i].at[0, c, pl.ds(row, 32)]
            remote(
                stages[i].at[:, pl.ds(col, 128)], dst, p1_send.at[i, half], p1_recv.at[i, half],
                dev(x, y1, z1 // 4, z1 % 4, c),
            ).start()
            return carry

        lax.fori_loop(1 - half, 16, send, 0)

    mycol = pl.ds(pl.multiple_of(p * 128, 128), 128)
    own = {}
    for i, half in ((0, 0), (1, 0), (2, 0), (2, 1), (0, 1), (1, 1)):
        if half == 0:
            stage[i].wait()
        send_half(i, half)
        if half == 0:
            dst = qbuf.at[pl.ds(qrow, 32)] if i == 2 else bufs[i].at[0, c, pl.ds(0, 32)]
            cp = pltpu.make_async_copy(stages[i].at[:, mycol], dst, s_loc.at[3 + i])
            cp.start()
            own[i] = cp

    tcol = pl.multiple_of((zl % 2) * 128, 128)
    texts = []
    for i, src in enumerate((tk_hbm, tv_hbm)):
        piece = src.at[:, pl.ds(tcol, 128)]
        cp = remote(piece, tbuf.at[i, c], t_send.at[i], t_recv.at[i], partner)
        cp.start()
        mine = pltpu.make_async_copy(piece, tbuf.at[i, c], s_loc.at[6 + i])
        mine.start()
        texts.append((cp, mine))

    wrow = pl.ds(pl.multiple_of(c * 256, 256), 256)

    def wcols(y1):
        return w_hbm.at[:, pl.ds(pl.multiple_of(y1 * COLS, 128), COLS)]

    wown = pltpu.make_async_copy(wcols(y), wbuf.at[y, wrow], s_loc.at[8])
    wown.start()
    wd = [remote(wcols(y), wbuf.at[y, wrow], wd_send.at[0], wd_recv.at[0], partner)]
    wd[0].start()
    ws = {}
    pair = zl + 1 - 2 * (zl % 2)
    hrow = pl.multiple_of((zl % 2) * 128, 128)
    y2 = (y + 2) % 4
    ws[2] = remote(
        w_hbm.at[pl.ds(hrow, 128), pl.ds(pl.multiple_of(y2 * COLS, 128), COLS)],
        wbuf.at[y, pl.ds(pl.multiple_of(c * 256 + hrow, 128), 128)],
        w_send.at[2], w_recv.at[2], dev(x, y2, zh, zl, c),
    )
    ws[2].start()
    for dy in (1, 3):
        y1 = (y + dy) % 4
        ws[dy] = remote(wcols(y1), wbuf.at[y, wrow], w_send.at[dy], w_recv.at[dy], dev(x, y1, zh, zl, c))
        ws[dy].start()

    def pass_pair():
        ws[2].wait_recv()
        piece = wbuf.at[y2, pl.ds(pl.multiple_of(c * 256 + hrow, 128), 128)]
        ws[4] = remote(piece, piece, w_send.at[4], w_recv.at[4], dev(x, y, zh, pair, c))
        ws[4].start()

    def total_wait(buf, sem):
        pltpu.make_async_copy(buf, buf, sem).wait()

    xs, ds = {}, {}

    def share(i, half, slot):
        return bufs[i].at[slot, c, pl.ds(half * 512, 512)]

    def send_x(i, half, src_slot, dst_slot, to):
        cp = remote(
            share(i, half, src_slot), share(i, half, dst_slot),
            x_send.at[i, half, dst_slot], x_recv.at[i, half, dst_slot], dev(to, y, zh, zl, c),
        )
        cp.start()
        xs[(i, half, dst_slot)] = cp

    def send_d(i, half, slot):
        cp = remote(
            share(i, half, slot), share(i, half, slot),
            d_send.at[i, half, slot], d_recv.at[i, half, slot], partner,
        )
        cp.start()
        ds[(i, half, slot)] = cp

    def arrive_own(i, half):
        if half == 0:
            own[i].wait()
        n = 480 if half == 0 else 512
        total_wait(bufs[i].at[0, c, pl.ds(0, n)], p1_recv.at[i, half])
        send_x(i, half, 0, 3, right)
        send_x(i, half, 0, 1, left)
        send_d(i, half, 0)

    def arrive_near(i, half):
        first, second = (3, 1) if i == 0 else (1, 3)
        xs[(i, half, first)].wait_recv()
        send_x(i, half, first, 2, right if i == 0 else left)
        send_d(i, half, first)
        xs[(i, half, second)].wait_recv()
        send_d(i, half, second)

    def arrive_far(half):
        for i in (0, 1):
            xs[(i, half, 2)].wait_recv()
            send_d(i, half, 2)

    def arrive_core(half, slot):
        for i in (0, 1):
            ds[(i, half, slot)].wait_recv()

    def step(row, nrow, pieces, first):
        rows = pl.ds(row, nrow)
        q = qbuf[rows, :]
        scs = [
            lax.dot_general(q, kk(), (((1,), (1,)), ((), ())), preferred_element_type=F32)
            for kk, vv in pieces
        ]
        lanes = [sc[:, i : i + 128] for sc in scs for i in range(0, sc.shape[1], 128)]
        m_new = jnp.max(functools.reduce(jnp.maximum, lanes), axis=1, keepdims=True)
        if first:
            m_new = jnp.broadcast_to(m_new, (nrow, 128))
        else:
            m_old = m_ref[rows, :]
            m_new = jnp.maximum(m_old, m_new)
        tot, o = None, None
        for sc, (kk, vv) in zip(scs, pieces):
            ws = []
            for i in range(0, sc.shape[1], 128):
                w = jnp.exp2((sc[:, i : i + 128] - m_new) * C2)
                tot = w if tot is None else tot + w
                ws.append(w.astype(BF))
            part_o = jnp.dot(jnp.concatenate(ws, axis=1), vv(), preferred_element_type=F32)
            o = part_o if o is None else o + part_o
        if first:
            acc[rows, :] = o
            l_ref[rows, :] = tot
        else:
            al = jnp.exp2((m_old - m_new) * C2)
            acc[rows, :] = acc[rows, :] * al + o
            l_ref[rows, :] = l_ref[rows, :] * al + tot
        m_ref[rows, :] = m_new

    src_core = zl // 2
    text_piece = (lambda: tbuf[0, src_core], lambda: tbuf[1, src_core])

    def video_pieces(half, slot):
        hr = pl.ds(half * 512, 512)
        return [
            (lambda core=core: kbuf[slot, core, hr], lambda core=core: vbuf[slot, core, hr])
            for core in range(2)
        ]

    def all_rows(pieces, first=False):
        def one(qi, carry):
            step(pl.multiple_of(qi * QB, QB), QB, pieces, first)
            return carry

        lax.fori_loop(0, 1024 // QB, one, 0)

    arrive_own(0, 0)
    arrive_own(1, 0)
    arrive_near(0, 0)
    arrive_near(1, 0)
    own[2].wait()
    total_wait(qbuf.at[pl.ds(0, 480)], p1_recv.at[2, 0])
    total_wait(qbuf.at[pl.ds(0, 512)], p1_recv.at[2, 1])
    for cp, mine in texts:
        mine.wait()
        cp.wait_recv()
    all_rows([text_piece], True)
    arrive_core(0, 0)
    all_rows(video_pieces(0, 0))
    arrive_own(0, 1)
    arrive_far(0)
    arrive_core(0, 1)
    all_rows(video_pieces(0, 1))
    arrive_own(1, 1)
    pass_pair()
    arrive_core(0, 3)
    all_rows(video_pieces(0, 3))
    arrive_near(0, 1)
    arrive_core(0, 2)
    all_rows(video_pieces(0, 2))
    arrive_near(1, 1)
    arrive_core(1, 0)
    all_rows(video_pieces(1, 0))
    arrive_core(1, 1)
    all_rows(video_pieces(1, 1))
    arrive_far(1)
    arrive_core(1, 3)
    all_rows(video_pieces(1, 3))

    wown.wait()
    for dy in (2, 1, 3):
        ws[4 if dy == 2 else dy].wait_recv()
        piece = wbuf.at[(y + 4 - dy) % 4, wrow]
        cp = remote(piece, piece, wd_send.at[dy], wd_recv.at[dy], partner)
        cp.start()
        wd.append(cp)
    arrive_core(1, 2)

    aas, bs = {}, {}
    mycols = pl.ds(pl.multiple_of(zl * 128, 128), 128)

    def last_rows(zhalf):
        row = pl.multiple_of(zhalf * 512, 512)
        step(row, 512, video_pieces(1, 2), False)
        rows = pl.ds(row, 512)
        att[rows, :] = (acc[rows, :] / jnp.sum(l_ref[rows, :], axis=1, keepdims=True)).astype(BF)

    def send_att(zhalf, k):
        for d in range(1, 4):
            zl1 = (zl + d) % 4
            rows = pl.ds(pl.multiple_of(zhalf * 512 + zl1 * 128, 128), 128)
            cp = remote(
                att.at[rows], abuf.at[zhalf, y, :, mycols], a_send.at[k, d], a_recv.at[k, d],
                dev(x, y, zh, zl1, c),
            )
            cp.start()
            aas[(k, d)] = cp
        rows = pl.ds(pl.multiple_of(zhalf * 512 + zl * 128, 128), 128)
        abuf[zhalf, y, :, mycols] = att[rows, :]

    def send_b(zhalf, k):
        for d in range(1, 4):
            aas[(k, d)].wait_recv()
        piece = abuf.at[zhalf, y]
        for dy in (2, 1, 3):
            cp = remote(
                piece, piece, b_send.at[k, dy], b_recv.at[k, dy], dev(x, (y + dy) % 4, zh, zl, c)
            )
            cp.start()
            bs[(k, dy)] = cp

    away, home = 1 - zh, zh
    last_rows(away)
    send_att(away, 0)
    last_rows(home)
    send_att(home, 1)
    send_b(away, 0)
    send_b(home, 1)

    for cp in wd:
        cp.wait_recv()

    def part(zhalf, n):
        tot = None
        for yy in range(4):
            t = jnp.dot(
                abuf[zhalf, yy], wbuf[yy, :, n * CW : (n + 1) * CW], preferred_element_type=F32
            )
            tot = t if tot is None else tot + t
        return tot

    for dy in range(1, 4):
        bs[(0, dy)].wait_recv()
    zs = []
    for n in range(NCH):
        psend[n] = part(away, n).astype(BF)
        cp = remote(psend.at[n], zbuf.at[n], z_send.at[n], z_recv.at[n], dev(x, y, 1 - zh, zl, c))
        cp.start()
        zs.append(cp)
    for dy in range(1, 4):
        bs[(1, dy)].wait_recv()
    for n in range(NCH):
        pown[n] = part(home, n)
    os = []
    for n in range(NCH):
        zs[n].wait_recv()
        osend[n] = (pown[n] + zbuf[n].astype(F32)).astype(BF)
        for dy in (2, 1, 3):
            y1 = (y + dy) % 4
            cp = remote(
                osend.at[n, pl.ds(pl.multiple_of(y1 * 32, 32), 32)],
                out_ref.at[:, pl.ds(pl.multiple_of(y * COLS + n * CW, 128), CW)],
                o_send.at[n, dy], o_recv.at[n, dy], dev(x, y1, zh, zl, c),
            )
            cp.start()
            os.append(cp)
        out_ref[:, pl.ds(pl.multiple_of(y * COLS + n * CW, 128), CW)] = osend[
            n, pl.ds(pl.multiple_of(y * 32, 32), 32), :
        ]

    for cp in os:
        cp.wait_recv()
    for i in range(3):
        for half in range(2):
            n = 480 if half == 0 else 512
            total_wait(qbuf.at[pl.ds(0, n)], p1_send.at[i, half])
    for cp in (
        [t[0] for t in texts] + list(ws.values()) + wd + list(xs.values()) + list(ds.values())
        + list(aas.values()) + list(bs.values()) + zs + os
    ):
        cp.wait_send()


def body(*args):
    dma = pltpu.SemaphoreType.DMA
    vm = pltpu.VMEM
    return pl.pallas_call(
        kernel,
        out_shape=jax.ShapeDtypeStruct((32, 5120), BF),
        in_specs=[pl.BlockSpec(memory_space=pl.ANY)] * 6,
        out_specs=pl.BlockSpec(memory_space=pltpu.VMEM),
        scratch_shapes=[
            vm((32, 4096), BF), vm((32, 4096), BF), vm((32, 4096), BF),
            vm((1024, 128), BF), vm((4, 2, 1024, 128), BF), vm((4, 2, 1024, 128), BF),
            vm((2, 2, 512, 128), BF), vm((4, 512, COLS), BF), vm((2, 4, 128, 512), BF),
            vm((1024, 128), BF), vm((1024, 128), F32), vm((1024, 128), F32), vm((1024, 128), F32),
            vm((NCH, 128, CW), BF), vm((NCH, 128, CW), F32), vm((NCH, 128, CW), BF), vm((NCH, 128, CW), BF),
            dma((9,)), dma((3, 2)), dma((3, 2)), dma((2, 2, 4)), dma((2, 2, 4)), dma((2, 2, 4)), dma((2, 2, 4)),
            dma((2,)), dma((2,)), dma((5,)), dma((5,)), dma((4,)), dma((4,)),
            dma((2, 4)), dma((2, 4)), dma((2, 4)), dma((2, 4)),
            dma((NCH,)), dma((NCH,)), dma((NCH, 4)), dma((NCH, 4)),
        ],
        compiler_params=pltpu.CompilerParams(
            collective_id=0, has_side_effects=True, vmem_limit_bytes=60 * 1024 * 1024
        ),
    )(*args)


def solution(mesh):
    rows = P(("seq", "head"), None)
    in_specs = (rows, rows, rows, P(None, "head"), P(None, "head"), P("head", None))
    return jax.shard_map(body, mesh=mesh, in_specs=in_specs, out_specs=rows, check_vma=False)
```

```python
import functools
import math

import jax
import jax.numpy as jnp
from jax import lax
from jax.experimental import pallas as pl
from jax.experimental.pallas import tpu as pltpu
from jax.sharding import PartitionSpec as P

HD = 128
C2 = HD ** (-0.5) * math.log2(math.e)
BF = jnp.bfloat16
F32 = jnp.float32
MESH = pl.DeviceIdType.MESH
COLS = 1280
QB = 512
CW = 256
NCH = COLS // CW


def kernel(
    q_hbm, k_hbm, v_hbm, tk_hbm, tv_hbm, w_hbm, out_ref,
    qs, ks, vs, qbuf, kbuf, vbuf, tbuf, wbuf, abuf, att, acc, m_ref, l_ref,
    psend, pown, zbuf, osend,
    s_loc, p1_send, p1_recv, x_send, x_recv, d_send, d_recv, t_send, t_recv,
    w_send, w_recv, wd_send, wd_recv, a_send, a_recv, b_send, b_recv,
    z_send, z_recv, o_send, o_recv,
):
    s, h = lax.axis_index("seq"), lax.axis_index("head")
    x, zl = s % 4, s // 4
    y, zh, c = h // 4, (h // 2) % 2, h % 2
    z = zh * 4 + zl
    p = y * 8 + z

    def dev(x1, y1, zh1, zl1, c1):
        return (zl1 * 4 + x1, y1 * 4 + zh1 * 2 + c1)

    left, right = (x + 3) % 4, (x + 1) % 4

    stage = []
    for i, (src, dst) in enumerate(((k_hbm, ks), (v_hbm, vs), (q_hbm, qs))):
        cp = pltpu.make_async_copy(src, dst, s_loc.at[i])
        cp.start()
        stage.append(cp)

    barrier = pltpu.get_barrier_semaphore()

    def greet(i, carry):
        pp = (p + i) % 32
        pl.semaphore_signal(
            barrier, inc=1, device_id=dev(x, pp // 8, (pp // 4) % 2, pp % 4, c), device_id_type=MESH
        )
        return carry

    lax.fori_loop(1, 32, greet, 0)
    for d in (dev(left, y, zh, zl, c), dev(right, y, zh, zl, c), dev(x, y, zh, zl, 1 - c)):
        pl.semaphore_signal(barrier, inc=1, device_id=d, device_id_type=MESH)
    pl.semaphore_wait(barrier, 34)

    def remote(src, dst, ss, rs, device):
        return pltpu.make_async_remote_copy(
            src_ref=src, dst_ref=dst, send_sem=ss, recv_sem=rs, device_id=device, device_id_type=MESH
        )

    partner = dev(x, y, zh, zl, 1 - c)
    qrow = pl.multiple_of(zh * 512 + zl * 128 + y * 32, 32)
    stages = {0: ks, 1: vs, 2: qs}
    bufs = (kbuf, vbuf)

    def send_half(i, half):
        def send(j, carry):
            dz, dy = (j // 4) * 2 + half, j % 4
            y1, z1 = (y + dy) % 4, (z + dz) % 8
            col = pl.multiple_of((y1 * 8 + z1) * 128, 128)
            row = pl.multiple_of(half * 512 + j * 32, 32)
            dst = qbuf.at[pl.ds(qrow, 32)] if i == 2 else bufs[i].at[0, c, pl.ds(row, 32)]
            remote(
                stages[i].at[:, pl.ds(col, 128)], dst, p1_send.at[i, half], p1_recv.at[i, half],
                dev(x, y1, z1 // 4, z1 % 4, c),
            ).start()
            return carry

        lax.fori_loop(1 - half, 16, send, 0)

    mycol = pl.ds(pl.multiple_of(p * 128, 128), 128)
    own = {}
    for i, half in ((0, 0), (1, 0), (2, 0), (2, 1), (0, 1), (1, 1)):
        if half == 0:
            stage[i].wait()
        send_half(i, half)
        if half == 0:
            dst = qbuf.at[pl.ds(qrow, 32)] if i == 2 else bufs[i].at[0, c, pl.ds(0, 32)]
            cp = pltpu.make_async_copy(stages[i].at[:, mycol], dst, s_loc.at[3 + i])
            cp.start()
            own[i] = cp

    tcol = pl.multiple_of((zl % 2) * 128, 128)
    texts = []
    for i, src in enumerate((tk_hbm, tv_hbm)):
        piece = src.at[:, pl.ds(tcol, 128)]
        cp = remote(piece, tbuf.at[i, c], t_send.at[i], t_recv.at[i], partner)
        cp.start()
        mine = pltpu.make_async_copy(piece, tbuf.at[i, c], s_loc.at[6 + i])
        mine.start()
        texts.append((cp, mine))

    wrow = pl.ds(pl.multiple_of(c * 256, 256), 256)

    def wcols(y1):
        return w_hbm.at[:, pl.ds(pl.multiple_of(y1 * COLS, 128), COLS)]

    wown = pltpu.make_async_copy(wcols(y), wbuf.at[y, wrow], s_loc.at[8])
    wown.start()
    wd = [remote(wcols(y), wbuf.at[y, wrow], wd_send.at[0], wd_recv.at[0], partner)]
    wd[0].start()
    ws = {}
    pair = zl + 1 - 2 * (zl % 2)
    hrow = pl.multiple_of((zl % 2) * 128, 128)
    y2 = (y + 2) % 4
    ws[2] = remote(
        w_hbm.at[pl.ds(hrow, 128), pl.ds(pl.multiple_of(y2 * COLS, 128), COLS)],
        wbuf.at[y, pl.ds(pl.multiple_of(c * 256 + hrow, 128), 128)],
        w_send.at[2], w_recv.at[2], dev(x, y2, zh, zl, c),
    )
    ws[2].start()
    for dy in (1, 3):
        y1 = (y + dy) % 4
        ws[dy] = remote(wcols(y1), wbuf.at[y, wrow], w_send.at[dy], w_recv.at[dy], dev(x, y1, zh, zl, c))
        ws[dy].start()

    def pass_pair():
        ws[2].wait_recv()
        piece = wbuf.at[y2, pl.ds(pl.multiple_of(c * 256 + hrow, 128), 128)]
        ws[4] = remote(piece, piece, w_send.at[4], w_recv.at[4], dev(x, y, zh, pair, c))
        ws[4].start()

    def total_wait(buf, sem):
        pltpu.make_async_copy(buf, buf, sem).wait()

    xs, ds = {}, {}

    def share(i, half, slot):
        return bufs[i].at[slot, c, pl.ds(half * 512, 512)]

    def send_x(i, half, src_slot, dst_slot, to):
        cp = remote(
            share(i, half, src_slot), share(i, half, dst_slot),
            x_send.at[i, half, dst_slot], x_recv.at[i, half, dst_slot], dev(to, y, zh, zl, c),
        )
        cp.start()
        xs[(i, half, dst_slot)] = cp

    def send_d(i, half, slot):
        cp = remote(
            share(i, half, slot), share(i, half, slot),
            d_send.at[i, half, slot], d_recv.at[i, half, slot], partner,
        )
        cp.start()
        ds[(i, half, slot)] = cp

    def arrive_own(i, half):
        if half == 0:
            own[i].wait()
        n = 480 if half == 0 else 512
        total_wait(bufs[i].at[0, c, pl.ds(0, n)], p1_recv.at[i, half])
        send_x(i, half, 0, 3, right)
        send_x(i, half, 0, 1, left)
        send_d(i, half, 0)

    def arrive_near(i, half):
        first, second = (3, 1) if i == 0 else (1, 3)
        xs[(i, half, first)].wait_recv()
        send_x(i, half, first, 2, right if i == 0 else left)
        send_d(i, half, first)
        xs[(i, half, second)].wait_recv()
        send_d(i, half, second)

    def arrive_far(half):
        for i in (0, 1):
            xs[(i, half, 2)].wait_recv()
            send_d(i, half, 2)

    def arrive_core(half, slot):
        for i in (0, 1):
            ds[(i, half, slot)].wait_recv()

    def step(row, nrow, pieces, first):
        rows = pl.ds(row, nrow)
        q = qbuf[rows, :]
        scs = [
            lax.dot_general(q, kk(), (((1,), (1,)), ((), ())), preferred_element_type=F32)
            for kk, vv in pieces
        ]
        lanes = [sc[:, i : i + 128] for sc in scs for i in range(0, sc.shape[1], 128)]
        m_new = jnp.max(functools.reduce(jnp.maximum, lanes), axis=1, keepdims=True)
        if first:
            m_new = jnp.broadcast_to(m_new, (nrow, 128))
        else:
            m_old = m_ref[rows, :]
            m_new = jnp.maximum(m_old, m_new)
        tot, o = None, None
        for sc, (kk, vv) in zip(scs, pieces):
            ws = []
            for i in range(0, sc.shape[1], 128):
                w = jnp.exp2((sc[:, i : i + 128] - m_new) * C2)
                tot = w if tot is None else tot + w
                ws.append(w.astype(BF))
            part_o = jnp.dot(jnp.concatenate(ws, axis=1), vv(), preferred_element_type=F32)
            o = part_o if o is None else o + part_o
        if first:
            acc[rows, :] = o
            l_ref[rows, :] = tot
        else:
            al = jnp.exp2((m_old - m_new) * C2)
            acc[rows, :] = acc[rows, :] * al + o
            l_ref[rows, :] = l_ref[rows, :] * al + tot
        m_ref[rows, :] = m_new

    src_core = zl // 2
    text_piece = (lambda: tbuf[0, src_core], lambda: tbuf[1, src_core])

    def video_pieces(half, slot):
        hr = pl.ds(half * 512, 512)
        return [
            (lambda core=core: kbuf[slot, core, hr], lambda core=core: vbuf[slot, core, hr])
            for core in range(2)
        ]

    away, home = 1 - zh, zh

    def attend(zhalf, half, slot):
        first = half == 0 and slot == 0
        pieces = ([text_piece] if first else []) + video_pieces(half, slot)
        step(pl.multiple_of(zhalf * 512, 512), 512, pieces, first)

    arrive_own(0, 0)
    arrive_own(1, 0)
    arrive_near(0, 0)
    arrive_near(1, 0)
    own[2].wait()
    total_wait(qbuf.at[pl.ds(0, 480)], p1_recv.at[2, 0])
    total_wait(qbuf.at[pl.ds(0, 512)], p1_recv.at[2, 1])
    for cp, mine in texts:
        mine.wait()
        cp.wait_recv()
    arrive_core(0, 0)
    attend(away, 0, 0)
    attend(home, 0, 0)
    arrive_own(0, 1)
    arrive_far(0)
    arrive_core(0, 1)
    attend(away, 0, 1)
    attend(home, 0, 1)
    arrive_own(1, 1)
    arrive_core(0, 3)
    attend(away, 0, 3)
    arrive_near(0, 1)
    attend(home, 0, 3)
    pass_pair()
    arrive_core(0, 2)
    attend(away, 0, 2)
    attend(home, 0, 2)
    arrive_near(1, 1)
    arrive_core(1, 0)
    attend(away, 1, 0)
    attend(home, 1, 0)
    arrive_core(1, 1)
    attend(away, 1, 1)
    arrive_core(1, 3)
    attend(away, 1, 3)
    arrive_far(1)
    attend(home, 1, 1)
    wown.wait()
    for dy in (1, 3, 2):
        ws[4 if dy == 2 else dy].wait_recv()
        piece = wbuf.at[(y + 4 - dy) % 4, wrow]
        cp = remote(piece, piece, wd_send.at[dy], wd_recv.at[dy], partner)
        cp.start()
        wd.append(cp)
    arrive_core(1, 2)

    parts = ((away, 0, 64), (away, 64, 64), (home, 0, 128))
    aas, bs = {}, {}
    mycols = pl.ds(pl.multiple_of(zl * 128, 128), 128)

    def last_rows(zhalf):
        attend(zhalf, 1, 2)
        rows = pl.ds(pl.multiple_of(zhalf * 512, 512), 512)
        att[rows, :] = (acc[rows, :] / jnp.sum(l_ref[rows, :], axis=1, keepdims=True)).astype(BF)

    def send_att(k):
        zhalf, r0, nr = parts[k]
        for d in (2, 1, 3):
            zl1 = (zl + d) % 4
            rows = pl.ds(pl.multiple_of(zhalf * 512 + zl1 * 128 + r0, 64), nr)
            cp = remote(
                att.at[rows], abuf.at[zhalf, y, pl.ds(r0, nr), mycols], a_send.at[k, d], a_recv.at[k, d],
                dev(x, y, zh, zl1, c),
            )
            cp.start()
            aas[(k, d)] = cp
        rows = pl.ds(pl.multiple_of(zhalf * 512 + zl * 128 + r0, 64), nr)
        abuf[zhalf, y, r0 : r0 + nr, mycols] = att[rows, :]

    def send_b(k):
        zhalf, r0, nr = parts[k]
        for d in (0, 1, 3, 2):
            if d:
                aas[(k, d)].wait_recv()
            cols = pl.ds(pl.multiple_of(((zl + 4 - d) % 4) * 128, 128), 128)
            piece = abuf.at[zhalf, y, pl.ds(r0, nr), cols]
            for dy in (2, 1, 3):
                cp = remote(
                    piece, piece, b_send.at[k, d, dy], b_recv.at[k, d, dy],
                    dev(x, (y + dy) % 4, zh, zl, c),
                )
                cp.start()
                bs[(k, d, dy)] = cp

    last_rows(away)
    send_att(0)
    send_att(1)
    attend(home, 1, 3)
    send_b(0)
    send_b(1)
    last_rows(home)
    send_att(2)

    send_b(2)

    for cp in wd:
        cp.wait_recv()

    def wait_b(k):
        for d in range(4):
            for dy in range(1, 4):
                bs[(k, d, dy)].wait_recv()

    def part(k, n):
        zhalf, r0, nr = parts[k]
        tot = None
        for yy in range(4):
            t = jnp.dot(
                abuf[zhalf, yy, r0 : r0 + nr], wbuf[yy, :, n * CW : (n + 1) * CW],
                preferred_element_type=F32,
            )
            tot = t if tot is None else tot + t
        return tot

    zs = {}
    for k in (0, 1):
        wait_b(k)
        for n in range(NCH):
            psend[k, n] = part(k, n).astype(BF)
            zs[(k, n)] = remote(
                psend.at[k, n], zbuf.at[k, n], z_send.at[k, n], z_recv.at[k, n],
                dev(x, y, 1 - zh, zl, c),
            )
            zs[(k, n)].start()
    wait_b(2)
    for n in range(NCH):
        pown[n] = part(2, n)
    os = {}
    for k in (0, 1):
        for n in range(NCH):
            cols = pl.ds(pl.multiple_of(y * COLS + n * CW, 128), CW)
            zs[(k, n)].wait_recv()
            osend[k, n] = (pown[n, k * 64 : (k + 1) * 64] + zbuf[k, n].astype(F32)).astype(BF)
            for dy in (2, 1, 3):
                y1 = (y + dy) % 4
                cp = remote(
                    osend.at[k, n, pl.ds(pl.multiple_of((y1 % 2) * 32, 32), 32)],
                    out_ref.at[:, cols], o_send.at[n, dy], o_recv.at[n, dy], dev(x, y1, zh, zl, c),
                )
                pl.when(y1 // 2 == k)(cp.start)
                os[(n, dy)] = cp

            @pl.when(y // 2 == k)
            def _(k=k, n=n, cols=cols):
                out_ref[:, cols] = osend[k, n, pl.ds(pl.multiple_of((y % 2) * 32, 32), 32), :]

    for cp in os.values():
        cp.wait_recv()
    for i in range(3):
        for half in range(2):
            n = 480 if half == 0 else 512
            total_wait(qbuf.at[pl.ds(0, n)], p1_send.at[i, half])
    for cp in (
        [t[0] for t in texts] + list(ws.values()) + wd + list(xs.values()) + list(ds.values())
        + list(aas.values()) + list(bs.values())
        + list(zs.values()) + list(os.values())
    ):
        cp.wait_send()


def body(*args):
    dma = pltpu.SemaphoreType.DMA
    vm = pltpu.VMEM
    return pl.pallas_call(
        kernel,
        out_shape=jax.ShapeDtypeStruct((32, 5120), BF),
        in_specs=[pl.BlockSpec(memory_space=pl.ANY)] * 6,
        out_specs=pl.BlockSpec(memory_space=pltpu.VMEM),
        scratch_shapes=[
            vm((32, 4096), BF), vm((32, 4096), BF), vm((32, 4096), BF),
            vm((1024, 128), BF), vm((4, 2, 1024, 128), BF), vm((4, 2, 1024, 128), BF),
            vm((2, 2, 512, 128), BF), vm((4, 512, COLS), BF), vm((2, 4, 128, 512), BF),
            vm((1024, 128), BF), vm((1024, 128), F32), vm((1024, 128), F32), vm((1024, 128), F32),
            vm((2, NCH, 64, CW), BF), vm((NCH, 128, CW), F32), vm((2, NCH, 64, CW), BF), vm((2, NCH, 64, CW), BF),
            dma((9,)), dma((3, 2)), dma((3, 2)), dma((2, 2, 4)), dma((2, 2, 4)), dma((2, 2, 4)), dma((2, 2, 4)),
            dma((2,)), dma((2,)), dma((5,)), dma((5,)), dma((4,)), dma((4,)),
            dma((3, 4)), dma((3, 4)), dma((3, 4, 4)), dma((3, 4, 4)),
            dma((2, NCH)), dma((2, NCH)), dma((NCH, 4)), dma((NCH, 4)),
        ],
        compiler_params=pltpu.CompilerParams(
            collective_id=0, has_side_effects=True, vmem_limit_bytes=60 * 1024 * 1024
        ),
    )(*args)


def solution(mesh):
    rows = P(("seq", "head"), None)
    in_specs = (rows, rows, rows, P(None, "head"), P(None, "head"), P("head", None))
    return jax.shard_map(body, mesh=mesh, in_specs=in_specs, out_specs=rows, check_vma=False)
```
